32 devices in a mesh: seq: 8 (over z, x), head: 4 (over y, core).
Axes of the slice: x: 2, y: 2, z: 4, core: 2. Of those that a mesh axis runs over, the one named last changes fastest.
Arguments:
- tokens: bfloat16 [2048, 2560], P(('seq', 'head')), may hold values from -6 to 6
- w_xz: bfloat16 [2560, 2, 5120], P(None, None, 'head'), may hold values from -0.125 to 0.125
- w_bc: bfloat16 [2560, 256], replicated, may hold values from -0.125 to 0.125
- w_dt: bfloat16 [2560, 80], P(None, 'head'), may hold values from -0.125 to 0.125
- dt_bias: float32 [80], P('head'), may hold values from -2 to 1
- a_log: float32 [80], P('head'), may hold values from -16 to 0
- conv_x: bfloat16 [4, 5120], P(None, 'head'), may hold values from -3 to 3
- conv_bc: bfloat16 [4, 256], replicated, may hold values from -3 to 3
- norm_gain: float32 [5120], P('head'), may hold values from 0.5 to 1.5
- w_out: bfloat16 [5120, 2560], P('head'), may hold values from -0.078125 to 0.078125
Outputs:
- layer_out: bfloat16 [2048, 2560], P(('seq', 'head'))
The draws below stay inside these ranges and needn't reach their ends.
All inputs are finite; a program needn't handle non-finite values.
Results may differ from the reference program's by a relative error of at most 0.02.
Values may be sent and summed in bfloat16 or wider, within the bound.
A program may use at most 64 MiB of HBM per device.

```python
import jax
import jax.numpy as jnp
from jax import lax

D = 2560
HEADS = 80
HEAD_DIM = 64
STATE = 128
SPAN = 256
CONV = 4
DI = 5120
TOKENS = 2048
N_HEAD = 4


def draw_a_log(key, part):
    key_pick, key_strong, key_weak = jax.random.split(jax.random.fold_in(key, 7), 3)
    keepers = 5
    lasting = jax.random.randint(key_pick, (HEADS,), 0, 10) < keepers
    strong = jax.random.uniform(key_strong, (HEADS,), jnp.float32, jnp.log(0.03), jnp.log(0.08))
    weak = jax.random.uniform(key_weak, (HEADS,), jnp.float32, jnp.log(0.2 / TOKENS), jnp.log(1.0 / TOKENS))
    return jnp.where(lasting, weak, strong).astype(jnp.float32)


def level_of(own_key, dims, cuts, smallest, top_value):
    factor_of = 1.0
    for dim, parts in cuts:
        draws = jax.random.uniform(jax.random.fold_in(jax.random.fold_in(own_key, 6), dim), (parts,), jnp.float32, smallest / len(cuts), top_value / len(cuts))
        factor_of = factor_of * jnp.repeat(jnp.exp(draws), dims[dim] // parts).reshape((-1,) + (1,) * (len(dims) - 1 - dim))
    return factor_of


def gaussian(rng, shape, spread, bound, shards=(), kind=jnp.bfloat16):
    values = jax.random.normal(rng, shape, jnp.float32) * spread
    if len(shards) > 0:
        values = level_of(rng, shape, shards, -0.22, 0.18) * values
    return jnp.clip(values, min=-bound, max=bound).astype(kind)


def setup_inputs(seed: int = 0) -> dict:
    arg_keys = jax.random.split(jax.random.key(seed), 11)
    tokens = gaussian(arg_keys[0], (TOKENS, D), 1.0, 6.0, ((0, 32),))
    w_xz = gaussian(arg_keys[1], (D, 2, DI), D ** -0.5, 0.125, ((2, 4),))
    w_bc = gaussian(arg_keys[2], (D, 2 * STATE), D ** -0.5, 0.125)
    w_dt = gaussian(arg_keys[3], (D, HEADS), D ** -0.5, 0.125, ((1, 4),))
    dt_bias = jnp.clip(-2.0 + 3.0 * jax.random.uniform(arg_keys[4], (HEADS,), jnp.float32) ** level_of(arg_keys[4], (HEADS,), ((0, 4),), -0.2, 0.2), -2.0, 1.0)
    a_log = draw_a_log(jax.random.fold_in(arg_keys[10], 71), 0)
    conv_x = gaussian(arg_keys[6], (CONV, DI), CONV ** -0.5, 3.0, ((1, 4),))
    conv_bc = gaussian(arg_keys[7], (CONV, 2 * STATE), CONV ** -0.5, 3.0)
    norm_gain = jnp.clip(1.0 + 0.1 * jax.random.normal(arg_keys[8], (DI,), jnp.float32), 0.5, 1.5)
    w_out = gaussian(arg_keys[9], (DI, D), DI ** -0.5, 0.078125, ((0, 4),))
    return dict(tokens=tokens, w_xz=w_xz, w_bc=w_bc, w_dt=w_dt, dt_bias=dt_bias, a_log=a_log, conv_x=conv_x, conv_bc=conv_bc, norm_gain=norm_gain, w_out=w_out)


def causal_mix(values, kernel):
    kernel_size = kernel.shape[0]
    row_count = values.shape[0]
    padded = jnp.concatenate([jnp.zeros((kernel_size - 1, values.shape[1]), values.dtype), values], axis=0)
    summed = jnp.zeros(values.shape, jnp.float32)
    for offset in range(kernel_size):
        summed = summed + kernel[offset].astype(jnp.float32) * padded[offset:offset + row_count].astype(jnp.float32)
    return jax.nn.silu(summed).astype(jnp.bfloat16)

def span_update(carried, inputs):
    value_block, b_block, c_block, step_block, decay_block = inputs
    block_len = value_block.shape[0]
    cumulative = jnp.cumsum(decay_block, axis=0)
    cum_heads = cumulative.T
    differ = cum_heads[:, :, None] - cum_heads[:, None, :]
    causal_mask = (jnp.arange(block_len)[:, None] >= jnp.arange(block_len)[None, :])[None]
    scores = jnp.dot(c_block, b_block.T, preferred_element_type=jnp.float32)
    weights = jnp.where(causal_mask, jnp.exp(jnp.where(causal_mask, differ, 0.0)), 0.0)
    weights = (weights * scores[None] * step_block.T[:, None, :]).astype(jnp.bfloat16).astype(jnp.float32)
    value_wide = value_block.astype(jnp.float32)
    c_wide = c_block.astype(jnp.float32)
    b_wide = b_block.astype(jnp.float32)
    start_state = carried.astype(jnp.bfloat16).astype(jnp.float32)
    inside = jnp.einsum('hts,shp->thp', weights, value_wide, precision=lax.Precision.HIGHEST)
    carried_out = jnp.exp(cumulative)[:, :, None] * jnp.einsum('tn,hpn->thp', c_wide, start_state, precision=lax.Precision.HIGHEST)
    final_decay = cumulative[-1]
    tail_weight = jnp.exp(final_decay[None] - cumulative) * step_block
    scaled = (tail_weight[:, :, None] * value_wide).astype(jnp.bfloat16).astype(jnp.float32)
    new_state = jnp.exp(final_decay)[:, None, None] * carried + jnp.einsum('shp,sn->hpn', scaled, b_wide, precision=lax.Precision.HIGHEST)
    return (new_state, inside + carried_out)

def reference(tokens, w_xz, w_bc, w_dt, dt_bias, a_log, conv_x, conv_bc, norm_gain, w_out):
    total_rows = tokens.shape[0]
    projected = jnp.dot(tokens, w_xz.reshape(D, 2 * DI), preferred_element_type=jnp.float32).astype(jnp.bfloat16)
    value_pre = projected[:, :DI]
    gate_pre = projected[:, DI:]
    bc_pre = jnp.dot(tokens, w_bc, preferred_element_type=jnp.float32).astype(jnp.bfloat16)
    step_size = jax.nn.softplus(jnp.dot(tokens, w_dt, preferred_element_type=jnp.float32) + dt_bias[None])
    values = causal_mix(value_pre, conv_x)
    bc_mixed = causal_mix(bc_pre, conv_bc)
    b_input = bc_mixed[:, :STATE]
    c_input = bc_mixed[:, STATE:]
    log_decay = step_size * (-jnp.exp(a_log))[None]
    blocks = total_rows // SPAN
    inputs = (values.reshape(blocks, SPAN, HEADS, HEAD_DIM), b_input.reshape(blocks, SPAN, STATE), c_input.reshape(blocks, SPAN, STATE), step_size.reshape(blocks, SPAN, HEADS), log_decay.reshape(blocks, SPAN, HEADS))
    _, outputs = lax.scan(span_update, jnp.zeros((HEADS, HEAD_DIM, STATE), jnp.float32), inputs)
    ssm_out = outputs.reshape(total_rows, DI)
    gated = ssm_out * jax.nn.silu(gate_pre.astype(jnp.float32))
    scale = lax.rsqrt(lax.optimization_barrier(jnp.sum(gated * gated, axis=1, keepdims=True)) / DI + 1.0)
    normed = (gated * scale * norm_gain[None]).astype(jnp.bfloat16)
    group_width = DI // N_HEAD
    groups = normed.reshape(total_rows, N_HEAD, group_width).transpose(1, 0, 2)
    weight_groups = w_out.reshape(N_HEAD, group_width, D)

    def add_group(running, group_pair):
        part_sum = jnp.dot(group_pair[0], group_pair[1], preferred_element_type=jnp.float32).astype(jnp.bfloat16)
        part_sum = lax.optimization_barrier(part_sum)
        return (running + part_sum.astype(jnp.float32), None)
    summed, _ = lax.scan(add_group, jnp.zeros((total_rows, D), jnp.float32), (groups, weight_groups))
    return summed.astype(jnp.bfloat16)
```

```python
import functools

import jax
import jax.numpy as jnp
from jax import lax
from jax.experimental import pallas as pl
from jax.experimental.pallas import tpu as pltpu
from jax.sharding import PartitionSpec as P

F32 = jnp.float32
BF16 = jnp.bfloat16
MESH = pl.DeviceIdType.MESH
HALO = 16
NK = 5
NJ = 5
NP = 5
NT = (((1,), (1,)), ((), ()))
TN = (((0,), (0,)), ((), ()))


def dot(a, b, dims=(((1,), (0,)), ((), ())), precision=None):
    return lax.dot_general(a, b, dims, precision=precision, preferred_element_type=F32)


def silu(v):
    return v / (1.0 + jnp.exp(-v))


def softplus(v):
    return jnp.maximum(v, 0.0) + jnp.log1p(jnp.exp(-jnp.abs(v)))


def kernel(
    n_seq, n_head,
    tokens, w_hbm, wbc, wdt, dtb, alog, cvx, cvbc, gain, wo_hbm,
    out,
    wbuf, wobuf, xbuf, xint, emat, acc, bcbuf, cstep, ccum, rstep, rcum, vals, masked,
    st, stb, ra, dmine, dpart, pin, pout, tpart, sin, yacc, gbuf, sqs, sqr, sqs2, sqr2, sqown,
    pbuf, s1, r1, s2, r2, own,
    wsem, wosem, halo_s, halo_r, core_s, core_r, y_s, y_r, f_s, f_r,
    d_s, d_r, a_s, a_r, c_s, c_r, t_s, t_r, q_s, q_r, q2_s, q2_r, e_s, e_r, g_s, g_r,
):
    s = lax.axis_index("seq")
    h = lax.axis_index("head")
    R, K = tokens.shape
    N = w_hbm.shape[2]
    HL = wdt.shape[0]
    hw = N // HL
    ny = n_head // 2
    y, c = h // 2, h % 2
    other = y * 2 + (1 - c)
    z, x = s // 2, s % 2
    nz = n_seq // 2
    rows = R * n_head
    full = rows + HALO
    kc = K // NK
    D = wo_hbm.shape[1]
    jc = D // NJ
    last = n_head - 1

    def remote(src, dst, ss, rs, ts, th):
        return pltpu.make_async_remote_copy(
            src_ref=src, dst_ref=dst, send_sem=ss, recv_sem=rs, device_id=(ts, th), device_id_type=MESH)

    wcp = [pltpu.make_async_copy(w_hbm.at[pl.ds(k * kc, kc)], wbuf.at[k], wsem.at[k]) for k in range(NK)]
    for cp in wcp:
        cp.start()
    wocp = [
        pltpu.make_async_copy(wo_hbm.at[:, pl.ds(j * jc, jc)], wobuf.at[j], wosem.at[j]) for j in range(NJ)
    ]
    for cp in wocp:
        cp.start()

    bar = pltpu.get_barrier_semaphore()

    def hello(ts, th):
        pl.semaphore_signal(bar, inc=1, device_id=(ts, th), device_id_type=MESH)

    for d in range(1, n_head):
        hello(s, (h + d) % n_head)
    mate = s + 1 - 2 * x
    hello(mate, h)

    @pl.when(z > 0)
    def _():
        hello(s - 2, h)

    @pl.when(z < nz - 1)
    def _():
        hello(s + 2, h)

    @pl.when(s > 0)
    def _():
        hello(s - 1, last)

    @pl.when(jnp.logical_and(h == last, s < n_seq - 1))
    def _():
        for d in range(n_head):
            hello(s + 1, d)

    wait = n_head + jnp.where(z > 0, 1, 0) + jnp.where(z < nz - 1, 1, 0) + jnp.where(s > 0, 1, 0)
    wait = wait + jnp.where(jnp.logical_and(h == last, s < n_seq - 1), n_head, 0)

    def block(hh):
        return pl.ds(pl.multiple_of(HALO + hh * R, 16), R)

    xbuf[block(h), :] = tokens[...]

    @pl.when(s == 0)
    def _():
        xbuf[0:HALO, :] = jnp.zeros((HALO, K), BF16)

    er = lax.broadcasted_iota(jnp.int32, (256, 512), 0)
    ec = lax.broadcasted_iota(jnp.int32, (256, 512), 1)
    emat[0] = jnp.where(ec == 2 * er, 1.0, 0.0).astype(BF16)
    emat[1] = jnp.where(ec == 2 * er + 1, 1.0, 0.0).astype(BF16)
    pl.semaphore_wait(bar, wait)

    @pl.when(jnp.logical_and(h == last, s < n_seq - 1))
    def _():
        for d in range(n_head):
            remote(tokens.at[pl.ds(R - HALO, HALO)], xbuf.at[pl.ds(0, HALO)], halo_s.at[d], halo_r,
                   s + 1, d).start()

    def core_copy(k):
        return remote(tokens.at[:, pl.ds(k * kc, kc)], xbuf.at[block(h), pl.ds(k * kc, kc)],
                      core_s.at[k], core_r.at[k], s, other)

    def y_copy(k, d):
        return remote(tokens.at[:, pl.ds(k * kc, kc)], xbuf.at[block(h), pl.ds(k * kc, kc)],
                      y_s.at[d, k], y_r.at[d, k], s, ((y + d) % ny) * 2 + c)

    def f_copy(k, d):
        part = xbuf.at[block(((y + ny - d) % ny) * 2 + c), pl.ds(k * kc, kc)]
        return remote(part, part, f_s.at[d, k], f_r.at[d, k], s, other)

    for k in range(NK):
        for d in range(1, ny):
            y_copy(k, d).start()
        core_copy(k).start()

    def forward(k):
        for d in range(1, ny):
            y_copy(k, d).wait_recv()
            f_copy(k, d).start()

    forward(0)

    @pl.when(s > 0)
    def _():
        remote(tokens.at[pl.ds(R - HALO, HALO)], xbuf.at[pl.ds(0, HALO)], halo_s.at[0], halo_r,
               s, h).wait_recv()

    for k in range(NK):
        if k + 1 < NK:
            forward(k + 1)
        core_copy(k).wait_recv()
        for d in range(1, ny):
            f_copy(k, d).wait_recv()
        for b in range(kc // 256):
            piece = xbuf[:, k * kc + b * 256:k * kc + (b + 1) * 256]
            xint[0:full, b * 512:(b + 1) * 512] = dot(piece, emat[0]).astype(BF16)
            xint[full:2 * full, b * 512:(b + 1) * 512] = dot(piece, emat[1]).astype(BF16)
        wcp[k].wait()

        def columns(n, _):
            cols = pl.ds(pl.multiple_of(n * 256, 128), 256)
            w = wbuf[k, :, :, cols].reshape(2 * kc, 256)
            got = dot(xint[...], w)
            if k == 0:
                acc[:, cols] = got
            else:
                acc[:, cols] += got
            return 0

        if N % 256 == 0:
            lax.fori_loop(0, N // 256, columns, 0)
        else:
            got = dot(xint[...], wbuf[k].reshape(2 * kc, N))
            acc[...] = got if k == 0 else acc[...] + got

    xs = xbuf[HALO:full, :]
    eye = (lax.broadcasted_iota(jnp.int32, (HL, HL), 0) == lax.broadcasted_iota(jnp.int32, (HL, HL), 1))
    brow = dtb[...]
    rrow = -jnp.exp(alog[...])
    bcol = jnp.sum(jnp.where(eye, brow, 0.0), axis=1, keepdims=True)
    rcol = jnp.sum(jnp.where(eye, rrow, 0.0), axis=1, keepdims=True)
    step_c = softplus(dot(xs, wdt[...], NT) + brow)
    step_r = softplus(dot(wdt[...], xs, NT) + bcol)
    ti = lax.broadcasted_iota(jnp.int32, (rows, rows), 0)
    si = lax.broadcasted_iota(jnp.int32, (rows, rows), 1)
    lower = jnp.where(ti >= si, 1.0, 0.0)
    cum_c = dot(lower, step_c * rrow, precision=lax.Precision.HIGHEST)
    cum_r = dot(step_r * rcol, lower, NT, precision=lax.Precision.HIGHEST)
    cstep[...] = step_c
    ccum[...] = cum_c
    rstep[...] = step_r
    rcum[...] = cum_r
    end_r = cum_r[:, rows - 1:rows]
    dmine[...] = jnp.broadcast_to(end_r, (HL, 128))
    dcopy = remote(dmine, dpart, d_s, d_r, mate, h)
    dcopy.start()

    bcbuf[...] = dot(xbuf[...], wbc[...])
    pre = bcbuf[...].astype(BF16).astype(F32)
    taps = cvbc[...].astype(F32)
    mixed = jnp.zeros((rows, pre.shape[1]), F32)
    n_tap = taps.shape[0]
    for k in range(n_tap):
        shift = n_tap - 1 - k
        moved = pltpu.roll(pre, shift, 0) if shift else pre
        mixed = mixed + taps[k:k + 1, :] * moved[HALO:full]
    mixed = silu(mixed).astype(BF16)
    sw = mixed.shape[1] // 2
    b_in = mixed[:, :sw]
    c_in = mixed[:, sw:]
    masked[...] = jnp.where(ti >= si, dot(c_in, b_in, NT), 0.0)

    lane = lax.broadcasted_iota(jnp.int32, (rows, 128), 1)
    hlane = lax.broadcasted_iota(jnp.int32, (rows, HL), 1)
    per = 128 // hw

    def pick(arr, i):
        return jnp.sum(jnp.where(hlane == i, arr, 0.0), axis=1, keepdims=True)

    def spread(arr, p):
        got = pick(arr, p * per)
        for i in range(1, per):
            got = jnp.where(lane >= i * hw, pick(arr, p * per + i), got)
        return jnp.broadcast_to(got, (rows, 128))

    def own_state(p, _):
        cols = pl.ds(pl.multiple_of(p * 128, 128), 128)
        pre = acc[0:full, cols].astype(BF16).astype(F32)
        taps = cvx[:, cols].astype(F32)
        mixed = jnp.zeros((rows, 128), F32)
        for k in range(n_tap):
            shift = n_tap - 1 - k
            moved = pltpu.roll(pre, shift, 0) if shift else pre
            mixed = mixed + taps[k:k + 1, :] * moved[HALO:full]
        v = silu(mixed).astype(BF16)
        vals[:, cols] = v
        cum = ccum[...]
        tail = jnp.exp(cum[rows - 1:rows, :] - cum) * cstep[...]
        scaled = (spread(tail, p) * v.astype(F32)).astype(BF16)
        got = dot(scaled, b_in, TN)
        st[cols, :] = got
        stb[cols, :] = got.astype(BF16)
        return 0

    n_pair = N // 128
    lax.fori_loop(0, n_pair, own_state, 0)

    half = N // 2
    pr = half // NP
    ph = pr // hw

    def piece(ref, which, i):
        return ref.at[pl.ds(pl.multiple_of(which * half + i * pr, 16), pr)]

    def a_copy(i):
        return remote(piece(stb, 1 - x, i), ra.at[i], a_s.at[i], a_r.at[i], mate, h)

    def c_copy(i):
        return remote(pout.at[i], pin.at[i], c_s.at[i], c_r.at[i], s + 2, h)

    def t_copy(i):
        return remote(tpart.at[i], piece(sin, x, i), t_s.at[i], t_r.at[i], mate, h)

    for i in range(NP):
        a_copy(i).start()

    def inside(p, _):
        cols = pl.ds(pl.multiple_of(p * 128, 128), 128)
        v = vals[:, cols]
        cum = ccum[...]
        total = None
        for i in range(per):
            head = p * per + i
            away = pick(cum, head) - rcum[pl.ds(head, 1), :]
            w = jnp.exp(jnp.minimum(away, 0.0)) * masked[...] * rstep[pl.ds(head, 1), :]
            got = dot(w.astype(BF16), v)
            total = got if i == 0 else jnp.where(lane >= i * hw, got, total)
        yacc[:, cols] = total
        return 0

    early = (n_pair * (z + 1)) // nz
    lax.fori_loop(0, early, inside, 0)

    dcopy.wait_recv()

    @pl.when(z == 0)
    def _():
        for i in range(NP):
            pin[i] = jnp.zeros((pr, sw), BF16)

    for i in range(NP):
        a_copy(i).wait_recv()

        @pl.when(z > 0)
        def _():
            c_copy(i).wait_recv()

        for g in range(ph):
            head = x * (half // hw) + i * ph + g
            part = pl.ds(g * hw, hw)
            mine = jnp.exp(dmine[pl.ds(head, 1), :])
            theirs = jnp.exp(dpart[pl.ds(head, 1), :])
            d0 = jnp.where(x == 0, mine, theirs)
            d1 = jnp.where(x == 0, theirs, mine)
            mst = st[pl.ds(pl.multiple_of(head * hw, hw), hw), :]
            tst = ra[i, part, :].astype(F32)
            first = jnp.where(x == 0, mst, tst)
            second = jnp.where(x == 0, tst, mst)
            start = pin[i, part, :].astype(F32)
            after = d0 * start + first
            pout[i, part, :] = (d1 * after + second).astype(BF16)
            tpart[i, part, :] = jnp.where(x == 0, after, start).astype(BF16)
            sin[pl.ds(pl.multiple_of(head * hw, hw), hw), :] = jnp.where(x == 0, start, after).astype(BF16)

        @pl.when(z < nz - 1)
        def _():
            c_copy(i).start()

        t_copy(i).start()

    lax.fori_loop(early, n_pair, inside, 0)

    for i in range(NP):
        t_copy(i).wait_recv()

    def gate_part(p, total):
        cols = pl.ds(pl.multiple_of(p * 128, 128), 128)
        from_state = dot(c_in, sin[cols, :], NT)
        ssm = yacc[:, cols] + spread(jnp.exp(ccum[...]), p) * from_state
        gate = acc[full + HALO:2 * full, cols].astype(BF16).astype(F32)
        gated = ssm * silu(gate)
        gbuf[:, cols] = (gated * gain[:, cols]).astype(BF16)
        return total + gated * gated

    squares = lax.fori_loop(0, n_pair, gate_part, jnp.zeros((rows, 128), F32))
    pbuf[:, 0:128] = jnp.broadcast_to(jnp.sum(squares, axis=1, keepdims=True), (rows, 128))

    def rows_of(yy, cc):
        return pl.ds(pl.multiple_of((yy * 2 + cc) * R, 16), R)

    for yy in range(ny):
        sqs[yy] = pbuf[rows_of(yy, 1 - c), 0:128]
        sqown[yy] = pbuf[rows_of(yy, c), 0:128]
    q_copy = remote(sqs, sqr, q_s, q_r, s, other)
    q_copy.start()

    def q2_copy(d):
        return remote(sqs2.at[d], sqr2.at[d], q2_s.at[d], q2_r.at[d], s, ((y + d) % ny) * 2 + c)

    def e_copy(j):
        return remote(s1.at[j], r1.at[j], e_s.at[j], e_r.at[j], s, other)

    def g_copy(j, d):
        return remote(s2.at[j, d], r2.at[j, d], g_s.at[j, d], g_r.at[j, d], s, ((y + d) % ny) * 2 + c)

    def product(j):
        wocp[j].wait()
        pbuf[...] = dot(gbuf[...], wobuf[j])
        for yy in range(ny):
            s1[j, yy] = pbuf[rows_of(yy, 1 - c), :].astype(BF16)
        e_copy(j).start()
        for yy in range(ny):
            own[j, yy] = pbuf[rows_of(yy, c), :]

    def pass_on(j):
        e_copy(j).wait_recv()
        for d in range(1, ny):
            yy = (y + d) % ny
            s2[j, d] = (own[j, yy] + r1[j, yy].astype(F32)).astype(BF16)
            g_copy(j, d).start()

    product(0)
    q_copy.wait_recv()
    for d in range(1, ny):
        yy = (y + d) % ny
        sqs2[d] = sqown[yy] + sqr[yy]
        q2_copy(d).start()
    for j in range(1, NJ):
        product(j)
        pass_on(j - 1)
    pass_on(NJ - 1)

    square = sqown[y] + sqr[y]
    for d in range(1, ny):
        q2_copy(d).wait_recv()
        square = square + sqr2[d]
    scale = lax.rsqrt(square[:, 0:1] / (N * n_head) + 1.0)
    for j in range(NJ):
        total = own[j, y] + r1[j, y].astype(F32)
        for d in range(1, ny):
            g_copy(j, d).wait_recv()
            total = total + r2[j, d].astype(F32)
        out[:, j * jc:(j + 1) * jc] = (total * scale).astype(BF16)

    @pl.when(jnp.logical_and(h == last, s < n_seq - 1))
    def _():
        for d in range(n_head):
            remote(tokens.at[pl.ds(R - HALO, HALO)], xbuf.at[pl.ds(0, HALO)], halo_s.at[d], halo_r,
                   s + 1, d).wait_send()

    for k in range(NK):
        core_copy(k).wait_send()
        for d in range(1, ny):
            y_copy(k, d).wait_send()
            f_copy(k, d).wait_send()
    dcopy.wait_send()
    for i in range(NP):
        a_copy(i).wait_send()
        t_copy(i).wait_send()

    @pl.when(z < nz - 1)
    def _():
        for i in range(NP):
            c_copy(i).wait_send()

    q_copy.wait_send()
    for d in range(1, ny):
        q2_copy(d).wait_send()
    for j in range(NJ):
        e_copy(j).wait_send()
        for d in range(1, ny):
            g_copy(j, d).wait_send()


def body(n_seq, n_head, tokens, w_xz, w_bc, w_dt, dt_bias, a_log, conv_x, conv_bc, norm_gain, w_out):
    R, K = tokens.shape
    N = w_xz.shape[2]
    HL = w_dt.shape[1]
    D = w_out.shape[1]
    bc = w_bc.shape[1]
    sw = bc // 2
    rows = R * n_head
    full = rows + HALO
    ny = n_head // 2
    kc, jc, pr = K // NK, D // NJ, N // 2 // NP
    V = pltpu.VMEM
    dma = pltpu.SemaphoreType.DMA
    vm = pl.BlockSpec(memory_space=pltpu.VMEM)
    anyspace = pl.BlockSpec(memory_space=pl.ANY)
    scratch = [
        V((NK, kc, 2, N), BF16), V((NJ, N, jc), BF16), V((full, K), BF16), V((2 * full, 2 * kc), BF16),
        V((2, 256, 512), BF16), V((2 * full, N), F32), V((full, bc), F32),
        V((rows, HL), F32), V((rows, HL), F32), V((HL, rows), F32), V((HL, rows), F32),
        V((rows, N), BF16), V((rows, rows), F32),
        V((N, sw), F32), V((N, sw), BF16), V((NP, pr, sw), BF16), V((HL, 128), F32), V((HL, 128), F32),
        V((NP, pr, sw), BF16), V((NP, pr, sw), BF16), V((NP, pr, sw), BF16), V((N, sw), BF16),
        V((rows, N), F32), V((rows, N), BF16),
        V((ny, R, 128), F32), V((ny, R, 128), F32), V((ny, R, 128), F32), V((ny, R, 128), F32),
        V((ny, R, 128), F32),
        V((rows, jc), F32), V((NJ, ny, R, jc), BF16), V((NJ, ny, R, jc), BF16),
        V((NJ, ny, R, jc), BF16), V((NJ, ny, R, jc), BF16), V((NJ, ny, R, jc), F32),
        dma((NK,)), dma((NJ,)), dma((n_head,)), dma, dma((NK,)), dma((NK,)),
        dma((ny, NK)), dma((ny, NK)), dma((ny, NK)), dma((ny, NK)),
        dma, dma, dma((NP,)), dma((NP,)), dma((NP,)), dma((NP,)), dma((NP,)), dma((NP,)),
        dma, dma, dma((ny,)), dma((ny,)), dma((NJ,)), dma((NJ,)), dma((NJ, ny)), dma((NJ, ny)),
    ]
    return pl.pallas_call(
        functools.partial(kernel, n_seq, n_head),
        out_shape=jax.ShapeDtypeStruct((R, D), BF16),
        in_specs=[vm, anyspace, vm, vm, vm, vm, vm, vm, vm, anyspace],
        out_specs=vm,
        scratch_shapes=scratch,
        compiler_params=pltpu.CompilerParams(
            collective_id=0, has_side_effects=True, vmem_limit_bytes=62 * 2**20),
    )(tokens, w_xz, w_bc, w_dt.T, dt_bias[None], a_log[None], conv_x, conv_bc, norm_gain[None], w_out)


def solution(mesh):
    in_specs = (
        P(("seq", "head"), None),
        P(None, None, "head"),
        P(),
        P(None, "head"),
        P("head"),
        P("head"),
        P(None, "head"),
        P(),
        P("head"),
        P("head", None),
    )
    out_specs = P(("seq", "head"), None)
    run = functools.partial(body, mesh.shape["seq"], mesh.shape["head"])
    return jax.shard_map(run, mesh=mesh, in_specs=in_specs, out_specs=out_specs, check_vma=False)
```

```python
import functools

import jax
import jax.numpy as jnp
from jax import lax
from jax.experimental import pallas as pl
from jax.experimental.pallas import tpu as pltpu
from jax.sharding import PartitionSpec as P

F32 = jnp.float32
BF16 = jnp.bfloat16
MESH = pl.DeviceIdType.MESH
HALO = 8
NK = 5
NJ = 5
NP = 5
NT = (((1,), (1,)), ((), ()))
TN = (((0,), (0,)), ((), ()))


def dot(a, b, dims=(((1,), (0,)), ((), ())), precision=None):
    return lax.dot_general(a, b, dims, precision=precision, preferred_element_type=F32)


def silu(v):
    return v / (1.0 + jnp.exp(-v))


def softplus(v):
    return jnp.maximum(v, 0.0) + jnp.log1p(jnp.exp(-jnp.abs(v)))


def kernel(
    n_seq, n_head,
    tokens, w_hbm, wbc_hbm, wdt, dtb, alog, cvx, cvbc, gain1, wo_hbm,
    out,
    wbuf, wobuf, wbc, gain, tailb, edge, esg, xbuf, xint, emat, acc, bcbuf, ccum, rstep, rcum, vals, masked,
    st, stb, ra, dmine, dpart, pin, pout, tpart, sin, yacc, gbuf, sqs, sqr, sqs2, sqr2, sqown,
    pbuf, s1, r1, s2, r2, own,
    wsem, wosem, bcsem, halo_s, halo_r, core_s, core_r, y_s, y_r, f_s, f_r,
    d_s, d_r, a_s, a_r, c_s, c_r, t_s, t_r, q_s, q_r, q2_s, q2_r, e_s, e_r, g_s, g_r,
):
    s = lax.axis_index("seq")
    h = lax.axis_index("head")
    R, K = tokens.shape
    N = w_hbm.shape[2]
    HL = wdt.shape[0]
    hw = N // HL
    ny = n_head // 2
    y, c = h // 2, h % 2
    other = y * 2 + (1 - c)
    z, x = s // 2, s % 2
    nz = n_seq // 2
    rows = R * n_head
    full = rows + HALO
    kc = K // NK
    D = wo_hbm.shape[1]
    jc = D // NJ
    last = n_head - 1
    wide = N // 2 if N % 256 == 0 else N

    def remote(src, dst, ss, rs, ts, th):
        return pltpu.make_async_remote_copy(
            src_ref=src, dst_ref=dst, send_sem=ss, recv_sem=rs, device_id=(ts, th), device_id_type=MESH)

    wcp = [pltpu.make_async_copy(w_hbm.at[pl.ds(k * kc, kc)], wbuf.at[k], wsem.at[k]) for k in range(NK)]
    for cp in wcp:
        cp.start()
    bccp = pltpu.make_async_copy(wbc_hbm, wbc, bcsem)
    bccp.start()
    wocp = [
        pltpu.make_async_copy(wo_hbm.at[:, pl.ds(j * jc, jc)], wobuf.at[j], wosem.at[j]) for j in range(NJ)
    ]
    for cp in wocp:
        cp.start()

    bar = pltpu.get_barrier_semaphore()

    def hello(ts, th):
        pl.semaphore_signal(bar, inc=1, device_id=(ts, th), device_id_type=MESH)

    for d in range(1, n_head):
        hello(s, (h + d) % n_head)
    mate = s + 1 - 2 * x
    hello(mate, h)

    @pl.when(z > 0)
    def _():
        hello(s - 2, h)

    @pl.when(z < nz - 1)
    def _():
        hello(s + 2, h)

    @pl.when(s > 0)
    def _():
        hello(s - 1, last)

    @pl.when(jnp.logical_and(h == last, s < n_seq - 1))
    def _():
        for d in range(n_head):
            hello(s + 1, d)

    wait = n_head + jnp.where(z > 0, 1, 0) + jnp.where(z < nz - 1, 1, 0) + jnp.where(s > 0, 1, 0)
    wait = wait + jnp.where(jnp.logical_and(h == last, s < n_seq - 1), n_head, 0)

    def block(hh):
        return pl.ds(pl.multiple_of(HALO + hh * R, 8), R)

    xbuf[block(h), :] = tokens[...]

    @pl.when(s == 0)
    def _():
        xbuf[0:HALO, :] = jnp.zeros((HALO, K), BF16)

    gain[...] = gain1[...].reshape(1, N)
    er = lax.broadcasted_iota(jnp.int32, (256, 512), 0)
    ec = lax.broadcasted_iota(jnp.int32, (256, 512), 1)
    emat[...] = jnp.where(ec == 2 * er, 1.0, 0.0).astype(BF16)
    pl.semaphore_wait(bar, wait)

    @pl.when(jnp.logical_and(h == last, s < n_seq - 1))
    def _():
        for d in range(n_head):
            remote(tokens.at[pl.ds(R - HALO, HALO)], xbuf.at[pl.ds(0, HALO)], halo_s.at[d], halo_r,
                   s + 1, d).start()

    def core_copy(k):
        return remote(tokens.at[:, pl.ds(k * kc, kc)], xbuf.at[block(h), pl.ds(k * kc, kc)],
                      core_s.at[k], core_r.at[k], s, other)

    def y_copy(k, d):
        return remote(tokens.at[:, pl.ds(k * kc, kc)], xbuf.at[block(h), pl.ds(k * kc, kc)],
                      y_s.at[d, k], y_r.at[d, k], s, ((y + d) % ny) * 2 + c)

    def f_copy(k, d):
        part = xbuf.at[block(((y + ny - d) % ny) * 2 + c), pl.ds(k * kc, kc)]
        return remote(part, part, f_s.at[d, k], f_r.at[d, k], s, other)

    for k in range(NK):
        for d in range(1, ny):
            y_copy(k, d).start()
        core_copy(k).start()

    def forward(k):
        for d in range(1, ny):
            y_copy(k, d).wait_recv()
            f_copy(k, d).start()

    forward(0)

    @pl.when(s > 0)
    def _():
        remote(tokens.at[pl.ds(R - HALO, HALO)], xbuf.at[pl.ds(0, HALO)], halo_s.at[0], halo_r,
               s, h).wait_recv()

    for k in range(NK):
        if k + 1 < NK:
            forward(k + 1)
        core_copy(k).wait_recv()
        for d in range(1, ny):
            f_copy(k, d).wait_recv()
        for b in range(kc // 256):
            piece = xbuf[:, k * kc + b * 256:k * kc + (b + 1) * 256]
            even = dot(piece, emat[...])
            xint[0:full, b * 512:(b + 1) * 512] = even.astype(BF16)
            for q in range(4):
                odd = pltpu.roll(even[:, q * 128:(q + 1) * 128], 1, 1)
                xint[full:2 * full, b * 512 + q * 128:b * 512 + (q + 1) * 128] = odd.astype(BF16)
        wcp[k].wait()

        def columns(n, _):
            cols = pl.ds(pl.multiple_of(n * wide, 128), wide)
            w = wbuf[k, :, :, cols].reshape(2 * kc, wide)
            got = dot(xint[...], w)
            if k == 0:
                acc[:, cols] = got
            else:
                acc[:, cols] += got
            return 0

        lax.fori_loop(0, N // wide, columns, 0)

    xs = xbuf[HALO:full, :]
    eye = (lax.broadcasted_iota(jnp.int32, (HL, HL), 0) == lax.broadcasted_iota(jnp.int32, (HL, HL), 1))
    brow = dtb[...]
    rrow = -jnp.exp(alog[...])
    bcol = jnp.sum(jnp.where(eye, brow, 0.0), axis=1, keepdims=True)
    rcol = jnp.sum(jnp.where(eye, rrow, 0.0), axis=1, keepdims=True)
    step_c = softplus(dot(xs, wdt[...], NT) + brow)
    step_r = softplus(dot(wdt[...], xs, NT) + bcol)
    ti = lax.broadcasted_iota(jnp.int32, (rows, rows), 0)
    si = lax.broadcasted_iota(jnp.int32, (rows, rows), 1)
    lower = jnp.where(ti >= si, 1.0, 0.0)
    cum_c = dot(lower, step_c * rrow, precision=lax.Precision.HIGHEST)
    cum_r = dot(step_r * rcol, lower, NT, precision=lax.Precision.HIGHEST)
    ccum[...] = cum_c
    rstep[...] = step_r
    rcum[...] = cum_r
    tailb[...] = jnp.exp(cum_c[rows - 1:rows, :] - cum_c) * step_c
    edge[...] = jnp.exp(cum_c)
    end_r = cum_r[:, rows - 1:rows]
    dmine[...] = jnp.broadcast_to(end_r, (HL, 128))
    dcopy = remote(dmine, dpart, d_s, d_r, mate, h)
    dcopy.start()

    bccp.wait()
    bcbuf[...] = dot(xbuf[...], wbc[...])
    pre = bcbuf[...].astype(BF16).astype(F32)
    taps = cvbc[...].astype(F32)
    mixed = jnp.zeros((rows, pre.shape[1]), F32)
    n_tap = taps.shape[0]
    for k in range(n_tap):
        shift = n_tap - 1 - k
        moved = pltpu.roll(pre, shift, 0) if shift else pre
        mixed = mixed + taps[k:k + 1, :] * moved[HALO:full]
    mixed = silu(mixed).astype(BF16)
    sw = mixed.shape[1] // 2
    b_in = mixed[:, :sw]
    c_in = mixed[:, sw:]
    masked[...] = jnp.where(ti >= si, dot(c_in, b_in, NT), 0.0)

    lane = lax.broadcasted_iota(jnp.int32, (rows, 128), 1)
    hlane = lax.broadcasted_iota(jnp.int32, (rows, HL), 1)
    per = 128 // hw

    def pick(arr, i):
        return jnp.sum(jnp.where(hlane == i, arr, 0.0), axis=1, keepdims=True)

    def spread(arr, p):
        got = pick(arr, p * per)
        for i in range(1, per):
            got = jnp.where(lane >= i * hw, pick(arr, p * per + i), got)
        return jnp.broadcast_to(got, (rows, 128))

    n_pair = N // 128

    def own_state(i, _):
        p = (i + (1 - x) * (n_pair // 2)) % n_pair
        cols = pl.ds(pl.multiple_of(p * 128, 128), 128)
        pre = acc[0:full, cols].astype(BF16).astype(F32)
        taps = cvx[:, cols].astype(F32)
        mixed = jnp.zeros((rows, 128), F32)
        for k in range(n_tap):
            shift = n_tap - 1 - k
            moved = pltpu.roll(pre, shift, 0) if shift else pre
            mixed = mixed + taps[k:k + 1, :] * moved[HALO:full]
        v = silu(mixed).astype(BF16)
        vals[:, cols] = v
        scaled = (spread(tailb[...], p) * v.astype(F32)).astype(BF16)
        got = dot(scaled, b_in, TN)
        st[cols, :] = got
        stb[cols, :] = got.astype(BF16)
        return 0

    lax.fori_loop(0, (n_pair + 1) // 2, own_state, 0)

    half = N // 2
    pr = half // NP
    ph = pr // hw

    def piece(ref, which, i):
        return ref.at[pl.ds(pl.multiple_of(which * half + i * pr, 16), pr)]

    def a_copy(i):
        return remote(piece(stb, 1 - x, i), ra.at[i], a_s.at[i], a_r.at[i], mate, h)

    def c_copy(i):
        return remote(pout.at[i], pin.at[i], c_s.at[i], c_r.at[i], s + 2, h)

    def t_copy(i):
        return remote(tpart.at[i], piece(sin, x, i), t_s.at[i], t_r.at[i], mate, h)

    for i in range(NP):
        a_copy(i).start()

    lax.fori_loop((n_pair + 1) // 2, n_pair, own_state, 0)

    def inside(p, _):
        cols = pl.ds(pl.multiple_of(p * 128, 128), 128)
        v = vals[:, cols]
        cum = ccum[...]
        total = None
        for i in range(per):
            head = p * per + i
            away = pick(cum, head) - rcum[pl.ds(head, 1), :]
            w = jnp.exp(jnp.minimum(away, 0.0)) * masked[...] * rstep[pl.ds(head, 1), :]
            got = dot(w.astype(BF16), v)
            total = got if i == 0 else jnp.where(lane >= i * hw, got, total)
        gate = silu(acc[full + HALO:2 * full, cols].astype(BF16).astype(F32))
        yacc[:, cols] = total * gate
        esg[:, cols] = spread(edge[...], p) * gate
        return 0

    early = (n_pair * (z + 1)) // nz
    lax.fori_loop(0, early, inside, 0)

    dcopy.wait_recv()

    @pl.when(z == 0)
    def _():
        for i in range(NP):
            pin[i] = jnp.zeros((pr, sw), BF16)

    for i in range(NP):
        a_copy(i).wait_recv()

        @pl.when(z > 0)
        def _():
            c_copy(i).wait_recv()

        for g in range(ph):
            head = x * (half // hw) + i * ph + g
            part = pl.ds(g * hw, hw)
            mine = jnp.exp(dmine[pl.ds(head, 1), :])
            theirs = jnp.exp(dpart[pl.ds(head, 1), :])
            d0 = jnp.where(x == 0, mine, theirs)
            d1 = jnp.where(x == 0, theirs, mine)
            mst = st[pl.ds(pl.multiple_of(head * hw, hw), hw), :]
            tst = ra[i, part, :].astype(F32)
            first = jnp.where(x == 0, mst, tst)
            second = jnp.where(x == 0, tst, mst)
            start = pin[i, part, :].astype(F32)
            after = d0 * start + first
            pout[i, part, :] = (d1 * after + second).astype(BF16)
            tpart[i, part, :] = jnp.where(x == 0, after, start).astype(BF16)
            sin[pl.ds(pl.multiple_of(head * hw, hw), hw), :] = jnp.where(x == 0, start, after).astype(BF16)

        @pl.when(z < nz - 1)
        def _():
            c_copy(i).start()

        t_copy(i).start()

    lax.fori_loop(early, n_pair, inside, 0)

    for i in range(NP):
        t_copy(i).wait_recv()

    def gate_part(p, total):
        cols = pl.ds(pl.multiple_of(p * 128, 128), 128)
        from_state = dot(c_in, sin[cols, :], NT)
        gated = yacc[:, cols] + esg[:, cols] * from_state
        gbuf[:, cols] = (gated * gain[:, cols]).astype(BF16)
        return total + gated * gated

    squares = lax.fori_loop(0, n_pair, gate_part, jnp.zeros((rows, 128), F32))
    pbuf[:, 0:128] = jnp.broadcast_to(jnp.sum(squares, axis=1, keepdims=True), (rows, 128))

    def rows_of(yy, cc):
        return pl.ds(pl.multiple_of((yy * 2 + cc) * R, 16), R)

    for yy in range(ny):
        sqs[yy] = pbuf[rows_of(yy, 1 - c), 0:128]
        sqown[yy] = pbuf[rows_of(yy, c), 0:128]
    q_copy = remote(sqs, sqr, q_s, q_r, s, other)
    q_copy.start()

    def q2_copy(d):
        return remote(sqs2.at[d], sqr2.at[d], q2_s.at[d], q2_r.at[d], s, ((y + d) % ny) * 2 + c)

    def e_copy(j):
        return remote(s1.at[j], r1.at[j], e_s.at[j], e_r.at[j], s, other)

    def g_copy(j, d):
        return remote(s2.at[j, d], r2.at[j, d], g_s.at[j, d], g_r.at[j, d], s, ((y + d) % ny) * 2 + c)

    def product(j):
        wocp[j].wait()
        pbuf[...] = dot(gbuf[...], wobuf[j])
        for yy in range(ny):
            s1[j, yy] = pbuf[rows_of(yy, 1 - c), :].astype(BF16)
        e_copy(j).start()
        for yy in range(ny):
            own[j, yy] = pbuf[rows_of(yy, c), :]

    def pass_on(j):
        e_copy(j).wait_recv()
        for d in range(1, ny):
            yy = (y + d) % ny
            s2[j, d] = (own[j, yy] + r1[j, yy].astype(F32)).astype(BF16)
            g_copy(j, d).start()

    product(0)
    q_copy.wait_recv()
    for d in range(1, ny):
        yy = (y + d) % ny
        sqs2[d] = sqown[yy] + sqr[yy]
        q2_copy(d).start()
    for j in range(1, NJ):
        product(j)
        pass_on(j - 1)
    pass_on(NJ - 1)

    square = sqown[y] + sqr[y]
    for d in range(1, ny):
        q2_copy(d).wait_recv()
        square = square + sqr2[d]
    scale = lax.rsqrt(square[:, 0:1] / (N * n_head) + 1.0)
    for j in range(NJ):
        total = own[j, y] + r1[j, y].astype(F32)
        for d in range(1, ny):
            g_copy(j, d).wait_recv()
            total = total + r2[j, d].astype(F32)
        out[:, j * jc:(j + 1) * jc] = (total * scale).astype(BF16)

    @pl.when(jnp.logical_and(h == last, s < n_seq - 1))
    def _():
        for d in range(n_head):
            remote(tokens.at[pl.ds(R - HALO, HALO)], xbuf.at[pl.ds(0, HALO)], halo_s.at[d], halo_r,
                   s + 1, d).wait_send()

    for k in range(NK):
        core_copy(k).wait_send()
        for d in range(1, ny):
            y_copy(k, d).wait_send()
            f_copy(k, d).wait_send()
    dcopy.wait_send()
    for i in range(NP):
        a_copy(i).wait_send()
        t_copy(i).wait_send()

    @pl.when(z < nz - 1)
    def _():
        for i in range(NP):
            c_copy(i).wait_send()

    q_copy.wait_send()
    for d in range(1, ny):
        q2_copy(d).wait_send()
    for j in range(NJ):
        e_copy(j).wait_send()
        for d in range(1, ny):
            g_copy(j, d).wait_send()


def body(n_seq, n_head, tokens, w_xz, w_bc, w_dt, dt_bias, a_log, conv_x, conv_bc, norm_gain, w_out):
    R, K = tokens.shape
    N = w_xz.shape[2]
    HL = w_dt.shape[1]
    D = w_out.shape[1]
    bc = w_bc.shape[1]
    sw = bc // 2
    rows = R * n_head
    full = rows + HALO
    ny = n_head // 2
    kc, jc, pr = K // NK, D // NJ, N // 2 // NP
    V = pltpu.VMEM
    dma = pltpu.SemaphoreType.DMA
    vm = pl.BlockSpec(memory_space=pltpu.VMEM)
    anyspace = pl.BlockSpec(memory_space=pl.ANY)
    scratch = [
        V((NK, kc, 2, N), BF16), V((NJ, N, jc), BF16), V((K, bc), BF16), V((1, N), F32),
        V((rows, HL), F32), V((rows, HL), F32), V((rows, N), F32), V((full, K), BF16), V((2 * full, 2 * kc), BF16),
        V((256, 512), BF16), V((2 * full, N), F32), V((full, bc), F32),
        V((rows, HL), F32), V((HL, rows), F32), V((HL, rows), F32),
        V((rows, N), BF16), V((rows, rows), F32),
        V((N, sw), F32), V((N, sw), BF16), V((NP, pr, sw), BF16), V((HL, 128), F32), V((HL, 128), F32),
        V((NP, pr, sw), BF16), V((NP, pr, sw), BF16), V((NP, pr, sw), BF16), V((N, sw), BF16),
        V((rows, N), F32), V((rows, N), BF16),
        V((ny, R, 128), F32), V((ny, R, 128), F32), V((ny, R, 128), F32), V((ny, R, 128), F32),
        V((ny, R, 128), F32),
        V((rows, jc), F32), V((NJ, ny, R, jc), BF16), V((NJ, ny, R, jc), BF16),
        V((NJ, ny, R, jc), BF16), V((NJ, ny, R, jc), BF16), V((NJ, ny, R, jc), F32),
        dma((NK,)), dma((NJ,)), dma, dma((n_head,)), dma, dma((NK,)), dma((NK,)),
        dma((ny, NK)), dma((ny, NK)), dma((ny, NK)), dma((ny, NK)),
        dma, dma, dma((NP,)), dma((NP,)), dma((NP,)), dma((NP,)), dma((NP,)), dma((NP,)),
        dma, dma, dma((ny,)), dma((ny,)), dma((NJ,)), dma((NJ,)), dma((NJ, ny)), dma((NJ, ny)),
    ]
    return pl.pallas_call(
        functools.partial(kernel, n_seq, n_head),
        out_shape=jax.ShapeDtypeStruct((R, D), BF16),
        in_specs=[vm, anyspace, anyspace, vm, vm, vm, vm, vm, vm, anyspace],
        out_specs=vm,
        scratch_shapes=scratch,
        compiler_params=pltpu.CompilerParams(
            collective_id=0, has_side_effects=True, vmem_limit_bytes=62 * 2**20),
    )(tokens, w_xz, w_bc, w_dt.T, dt_bias[None], a_log[None], conv_x, conv_bc, norm_gain, w_out)


def solution(mesh):
    in_specs = (
        P(("seq", "head"), None),
        P(None, None, "head"),
        P(),
        P(None, "head"),
        P("head"),
        P("head"),
        P(None, "head"),
        P(),
        P("head"),
        P("head", None),
    )
    out_specs = P(("seq", "head"), None)
    run = functools.partial(body, mesh.shape["seq"], mesh.shape["head"])
    return jax.shard_map(run, mesh=mesh, in_specs=in_specs, out_specs=out_specs, check_vma=False)
```

```python
import functools

import jax
import jax.numpy as jnp
from jax import lax
from jax.experimental import pallas as pl
from jax.experimental.pallas import tpu as pltpu
from jax.sharding import PartitionSpec as P

F32 = jnp.float32
BF16 = jnp.bfloat16
MESH = pl.DeviceIdType.MESH
HALO = 8
NK = 5
NJ = 5
NP = 5
NT = (((1,), (1,)), ((), ()))
TN = (((0,), (0,)), ((), ()))


def dot(a, b, dims=(((1,), (0,)), ((), ())), precision=None):
    return lax.dot_general(a, b, dims, precision=precision, preferred_element_type=F32)


def silu(v):
    return v / (1.0 + jnp.exp(-v))


def softplus(v):
    return jnp.maximum(v, 0.0) + jnp.log1p(jnp.exp(-jnp.abs(v)))


def kernel(
    n_seq, n_head,
    tokens, w_hbm, wbc_hbm, wdt, dtb, alog, cvx, cvbc, gain1, wo_hbm,
    out,
    wbuf, wobuf, wbc, gain, tailb, edge, esg, xbuf, xint, xodd, gacc, emat, acc, bcbuf, ccum, rstep, rcum, vals, masked,
    st, stb, ra, dmine, dpart, pin, pout, tpart, sin, yacc, gbuf, sqs, sqr, sqs2, sqr2, sqown,
    pbuf, s1, r1, s2, r2, own,
    wsem, wosem, bcsem, halo_s, halo_r, core_s, core_r, y_s, y_r, f_s, f_r,
    d_s, d_r, a_s, a_r, c_s, c_r, t_s, t_r, q_s, q_r, q2_s, q2_r, e_s, e_r, g_s, g_r,
):
    s = lax.axis_index("seq")
    h = lax.axis_index("head")
    R, K = tokens.shape
    N = w_hbm.shape[2]
    HL = wdt.shape[0]
    hw = N // HL
    ny = n_head // 2
    y, c = h // 2, h % 2
    other = y * 2 + (1 - c)
    z, x = s // 2, s % 2
    nz = n_seq // 2
    rows = R * n_head
    full = rows + HALO
    kc = K // NK
    D = wo_hbm.shape[1]
    jc = D // NJ
    last = n_head - 1
    wide = N // 2 if N % 256 == 0 else N

    def remote(src, dst, ss, rs, ts, th):
        return pltpu.make_async_remote_copy(
            src_ref=src, dst_ref=dst, send_sem=ss, recv_sem=rs, device_id=(ts, th), device_id_type=MESH)

    wcp = [pltpu.make_async_copy(w_hbm.at[pl.ds(k * kc, kc)], wbuf.at[k], wsem.at[k]) for k in range(NK)]
    for cp in wcp:
        cp.start()
    bccp = pltpu.make_async_copy(wbc_hbm, wbc, bcsem)
    bccp.start()
    wocp = [
        pltpu.make_async_copy(wo_hbm.at[:, pl.ds(j * jc, jc)], wobuf.at[j], wosem.at[j]) for j in range(NJ)
    ]
    for cp in wocp:
        cp.start()

    bar = pltpu.get_barrier_semaphore()

    def hello(ts, th):
        pl.semaphore_signal(bar, inc=1, device_id=(ts, th), device_id_type=MESH)

    for d in range(1, n_head):
        hello(s, (h + d) % n_head)
    mate = s + 1 - 2 * x
    hello(mate, h)

    @pl.when(z > 0)
    def _():
        hello(s - 2, h)

    @pl.when(z < nz - 1)
    def _():
        hello(s + 2, h)

    @pl.when(s > 0)
    def _():
        hello(s - 1, last)

    @pl.when(jnp.logical_and(h == last, s < n_seq - 1))
    def _():
        for d in range(n_head):
            hello(s + 1, d)

    wait = n_head + jnp.where(z > 0, 1, 0) + jnp.where(z < nz - 1, 1, 0) + jnp.where(s > 0, 1, 0)
    wait = wait + jnp.where(jnp.logical_and(h == last, s < n_seq - 1), n_head, 0)

    def block(hh):
        return pl.ds(pl.multiple_of(HALO + hh * R, 8), R)

    xbuf[block(h), :] = tokens[...]

    @pl.when(s == 0)
    def _():
        xbuf[0:HALO, :] = jnp.zeros((HALO, K), BF16)

    gain[...] = gain1[...].reshape(1, N)
    er = lax.broadcasted_iota(jnp.int32, (256, 512), 0)
    ec = lax.broadcasted_iota(jnp.int32, (256, 512), 1)
    emat[...] = jnp.where(ec == 2 * er, 1.0, 0.0).astype(BF16)
    pl.semaphore_wait(bar, wait)

    @pl.when(jnp.logical_and(h == last, s < n_seq - 1))
    def _():
        for d in range(n_head):
            remote(tokens.at[pl.ds(R - HALO, HALO)], xbuf.at[pl.ds(0, HALO)], halo_s.at[d], halo_r,
                   s + 1, d).start()

    def core_copy(k):
        return remote(tokens.at[:, pl.ds(k * kc, kc)], xbuf.at[block(h), pl.ds(k * kc, kc)],
                      core_s.at[k], core_r.at[k], s, other)

    def y_copy(k, d):
        return remote(tokens.at[:, pl.ds(k * kc, kc)], xbuf.at[block(h), pl.ds(k * kc, kc)],
                      y_s.at[d, k], y_r.at[d, k], s, ((y + d) % ny) * 2 + c)

    def f_copy(k, d):
        part = xbuf.at[block(((y + ny - d) % ny) * 2 + c), pl.ds(k * kc, kc)]
        return remote(part, part, f_s.at[d, k], f_r.at[d, k], s, other)

    for k in range(NK):
        for d in range(1, ny):
            y_copy(k, d).start()
        core_copy(k).start()

    def forward(k):
        for d in range(1, ny):
            y_copy(k, d).wait_recv()
            f_copy(k, d).start()

    forward(0)

    @pl.when(s > 0)
    def _():
        remote(tokens.at[pl.ds(R - HALO, HALO)], xbuf.at[pl.ds(0, HALO)], halo_s.at[0], halo_r,
               s, h).wait_recv()

    for k in range(NK):
        if k + 1 < NK:
            forward(k + 1)
        core_copy(k).wait_recv()
        for d in range(1, ny):
            f_copy(k, d).wait_recv()
        for b in range(kc // 256):
            piece = xbuf[:, k * kc + b * 256:k * kc + (b + 1) * 256]
            even = dot(piece, emat[...])
            xint[:, b * 512:(b + 1) * 512] = even.astype(BF16)
            for q in range(4):
                odd = pltpu.roll(even[:, q * 128:(q + 1) * 128], 1, 1)
                xodd[k, :, b * 512 + q * 128:b * 512 + (q + 1) * 128] = odd[HALO:full].astype(BF16)
        wcp[k].wait()

        def columns(n, _):
            cols = pl.ds(pl.multiple_of(n * wide, 128), wide)
            w = wbuf[k, :, :, cols].reshape(2 * kc, wide)
            got = dot(xint[...], w)
            if k == 0:
                acc[:, cols] = got
            else:
                acc[:, cols] += got
            return 0

        lax.fori_loop(0, N // wide, columns, 0)

    xs = xbuf[HALO:full, :]
    eye = (lax.broadcasted_iota(jnp.int32, (HL, HL), 0) == lax.broadcasted_iota(jnp.int32, (HL, HL), 1))
    brow = dtb[...]
    rrow = -jnp.exp(alog[...])
    bcol = jnp.sum(jnp.where(eye, brow, 0.0), axis=1, keepdims=True)
    rcol = jnp.sum(jnp.where(eye, rrow, 0.0), axis=1, keepdims=True)
    step_c = softplus(dot(xs, wdt[...], NT) + brow)
    step_r = softplus(dot(wdt[...], xs, NT) + bcol)
    ti = lax.broadcasted_iota(jnp.int32, (rows, rows), 0)
    si = lax.broadcasted_iota(jnp.int32, (rows, rows), 1)
    lower = jnp.where(ti >= si, 1.0, 0.0)
    cum_c = dot(lower, step_c * rrow, precision=lax.Precision.HIGHEST)
    cum_r = dot(step_r * rcol, lower, NT, precision=lax.Precision.HIGHEST)
    ccum[...] = cum_c
    rstep[...] = step_r
    rcum[...] = cum_r
    tailb[...] = jnp.exp(cum_c[rows - 1:rows, :] - cum_c) * step_c
    edge[...] = jnp.exp(cum_c)
    end_r = cum_r[:, rows - 1:rows]
    dmine[...] = jnp.broadcast_to(end_r, (HL, 128))
    dcopy = remote(dmine, dpart, d_s, d_r, mate, h)
    dcopy.start()

    bccp.wait()
    bcbuf[...] = dot(xbuf[...], wbc[...])
    pre = bcbuf[...].astype(BF16).astype(F32)
    taps = cvbc[...].astype(F32)
    mixed = jnp.zeros((rows, pre.shape[1]), F32)
    n_tap = taps.shape[0]
    for k in range(n_tap):
        shift = n_tap - 1 - k
        moved = pltpu.roll(pre, shift, 0) if shift else pre
        mixed = mixed + taps[k:k + 1, :] * moved[HALO:full]
    mixed = silu(mixed).astype(BF16)
    sw = mixed.shape[1] // 2
    b_in = mixed[:, :sw]
    c_in = mixed[:, sw:]
    masked[...] = jnp.where(ti >= si, dot(c_in, b_in, NT), 0.0)

    lane = lax.broadcasted_iota(jnp.int32, (rows, 128), 1)
    hlane = lax.broadcasted_iota(jnp.int32, (rows, HL), 1)
    per = 128 // hw

    def pick(arr, i):
        return jnp.sum(jnp.where(hlane == i, arr, 0.0), axis=1, keepdims=True)

    def spread(arr, p):
        got = pick(arr, p * per)
        for i in range(1, per):
            got = jnp.where(lane >= i * hw, pick(arr, p * per + i), got)
        return jnp.broadcast_to(got, (rows, 128))

    n_pair = N // 128

    def own_state(i, _):
        p = (i + (1 - x) * (n_pair // 2)) % n_pair
        cols = pl.ds(pl.multiple_of(p * 128, 128), 128)
        pre = acc[0:full, cols].astype(BF16).astype(F32)
        taps = cvx[:, cols].astype(F32)
        mixed = jnp.zeros((rows, 128), F32)
        for k in range(n_tap):
            shift = n_tap - 1 - k
            moved = pltpu.roll(pre, shift, 0) if shift else pre
            mixed = mixed + taps[k:k + 1, :] * moved[HALO:full]
        v = silu(mixed).astype(BF16)
        vals[:, cols] = v
        scaled = (spread(tailb[...], p) * v.astype(F32)).astype(BF16)
        got = dot(scaled, b_in, TN)
        st[cols, :] = got
        stb[cols, :] = got.astype(BF16)
        return 0

    lax.fori_loop(0, (n_pair + 1) // 2, own_state, 0)

    half = N // 2
    pr = half // NP
    ph = pr // hw

    def piece(ref, which, i):
        return ref.at[pl.ds(pl.multiple_of(which * half + i * pr, 16), pr)]

    def a_copy(i):
        return remote(piece(stb, 1 - x, i), ra.at[i], a_s.at[i], a_r.at[i], mate, h)

    def c_copy(i):
        return remote(pout.at[i], pin.at[i], c_s.at[i], c_r.at[i], s + 2, h)

    def t_copy(i):
        return remote(tpart.at[i], piece(sin, x, i), t_s.at[i], t_r.at[i], mate, h)

    for i in range(NP):
        a_copy(i).start()

    lax.fori_loop((n_pair + 1) // 2, n_pair, own_state, 0)

    def inside(p, _):
        cols = pl.ds(pl.multiple_of(p * 128, 128), 128)
        v = vals[:, cols]
        cum = ccum[...]
        total = None
        for i in range(per):
            head = p * per + i
            away = pick(cum, head) - rcum[pl.ds(head, 1), :]
            w = jnp.exp(jnp.minimum(away, 0.0)) * masked[...] * rstep[pl.ds(head, 1), :]
            got = dot(w.astype(BF16), v)
            total = got if i == 0 else jnp.where(lane >= i * hw, got, total)
        gate = silu(gacc[:, cols].astype(BF16).astype(F32))
        yacc[:, cols] = total * gate
        esg[:, cols] = spread(edge[...], p) * gate
        return 0

    gw = 256 if N % 256 == 0 else 128

    def gates(n, _):
        cols = pl.ds(pl.multiple_of(n * gw, 128), gw)
        got = dot(xodd[0], wbuf[0, :, :, cols].reshape(2 * kc, gw))
        for k in range(1, NK):
            got = got + dot(xodd[k], wbuf[k, :, :, cols].reshape(2 * kc, gw))
        gacc[:, cols] = got
        return 0

    early = (n_pair * (z + 1)) // nz
    early_g = (early * 128 + gw - 1) // gw
    lax.fori_loop(0, early_g, gates, 0)
    lax.fori_loop(0, early, inside, 0)

    dcopy.wait_recv()

    @pl.when(z == 0)
    def _():
        for i in range(NP):
            pin[i] = jnp.zeros((pr, sw), BF16)

    for i in range(NP):
        a_copy(i).wait_recv()

        @pl.when(z > 0)
        def _():
            c_copy(i).wait_recv()

        for g in range(ph):
            head = x * (half // hw) + i * ph + g
            part = pl.ds(g * hw, hw)
            mine = jnp.exp(dmine[pl.ds(head, 1), :])
            theirs = jnp.exp(dpart[pl.ds(head, 1), :])
            d0 = jnp.where(x == 0, mine, theirs)
            d1 = jnp.where(x == 0, theirs, mine)
            mst = st[pl.ds(pl.multiple_of(head * hw, hw), hw), :]
            tst = ra[i, part, :].astype(F32)
            first = jnp.where(x == 0, mst, tst)
            second = jnp.where(x == 0, tst, mst)
            start = pin[i, part, :].astype(F32)
            after = d0 * start + first
            pout[i, part, :] = (d1 * after + second).astype(BF16)
            tpart[i, part, :] = jnp.where(x == 0, after, start).astype(BF16)
            sin[pl.ds(pl.multiple_of(head * hw, hw), hw), :] = jnp.where(x == 0, start, after).astype(BF16)

        @pl.when(z < nz - 1)
        def _():
            c_copy(i).start()

        t_copy(i).start()

    lax.fori_loop(early_g, N // gw, gates, 0)
    lax.fori_loop(early, n_pair, inside, 0)

    for i in range(NP):
        t_copy(i).wait_recv()

    def gate_part(p, total):
        cols = pl.ds(pl.multiple_of(p * 128, 128), 128)
        from_state = dot(c_in, sin[cols, :], NT)
        gated = yacc[:, cols] + esg[:, cols] * from_state
        gbuf[:, cols] = (gated * gain[:, cols]).astype(BF16)
        return total + gated * gated

    squares = lax.fori_loop(0, n_pair, gate_part, jnp.zeros((rows, 128), F32))
    pbuf[:, 0:128] = jnp.broadcast_to(jnp.sum(squares, axis=1, keepdims=True), (rows, 128))

    def rows_of(yy, cc):
        return pl.ds(pl.multiple_of((yy * 2 + cc) * R, 16), R)

    for yy in range(ny):
        sqs[yy] = pbuf[rows_of(yy, 1 - c), 0:128]
        sqown[yy] = pbuf[rows_of(yy, c), 0:128]
    q_copy = remote(sqs, sqr, q_s, q_r, s, other)
    q_copy.start()

    def q2_copy(d):
        return remote(sqs2.at[d], sqr2.at[d], q2_s.at[d], q2_r.at[d], s, ((y + d) % ny) * 2 + c)

    def e_copy(j):
        return remote(s1.at[j], r1.at[j], e_s.at[j], e_r.at[j], s, other)

    def g_copy(j, d):
        return remote(s2.at[j, d], r2.at[j, d], g_s.at[j, d], g_r.at[j, d], s, ((y + d) % ny) * 2 + c)

    def product(j):
        wocp[j].wait()
        pbuf[...] = dot(gbuf[...], wobuf[j])
        for yy in range(ny):
            s1[j, yy] = pbuf[rows_of(yy, 1 - c), :].astype(BF16)
        e_copy(j).start()
        for yy in range(ny):
            own[j, yy] = pbuf[rows_of(yy, c), :]

    def pass_on(j):
        e_copy(j).wait_recv()
        for d in range(1, ny):
            yy = (y + d) % ny
            s2[j, d] = (own[j, yy] + r1[j, yy].astype(F32)).astype(BF16)
            g_copy(j, d).start()

    product(0)
    q_copy.wait_recv()
    for d in range(1, ny):
        yy = (y + d) % ny
        sqs2[d] = sqown[yy] + sqr[yy]
        q2_copy(d).start()
    for j in range(1, NJ):
        product(j)
        pass_on(j - 1)
    pass_on(NJ - 1)

    square = sqown[y] + sqr[y]
    for d in range(1, ny):
        q2_copy(d).wait_recv()
        square = square + sqr2[d]
    scale = lax.rsqrt(square[:, 0:1] / (N * n_head) + 1.0)
    for j in range(NJ):
        total = own[j, y] + r1[j, y].astype(F32)
        for d in range(1, ny):
            g_copy(j, d).wait_recv()
            total = total + r2[j, d].astype(F32)
        out[:, j * jc:(j + 1) * jc] = (total * scale).astype(BF16)

    @pl.when(jnp.logical_and(h == last, s < n_seq - 1))
    def _():
        for d in range(n_head):
            remote(tokens.at[pl.ds(R - HALO, HALO)], xbuf.at[pl.ds(0, HALO)], halo_s.at[d], halo_r,
                   s + 1, d).wait_send()

    for k in range(NK):
        core_copy(k).wait_send()
        for d in range(1, ny):
            y_copy(k, d).wait_send()
            f_copy(k, d).wait_send()
    dcopy.wait_send()
    for i in range(NP):
        a_copy(i).wait_send()
        t_copy(i).wait_send()

    @pl.when(z < nz - 1)
    def _():
        for i in range(NP):
            c_copy(i).wait_send()

    q_copy.wait_send()
    for d in range(1, ny):
        q2_copy(d).wait_send()
    for j in range(NJ):
        e_copy(j).wait_send()
        for d in range(1, ny):
            g_copy(j, d).wait_send()


def body(n_seq, n_head, tokens, w_xz, w_bc, w_dt, dt_bias, a_log, conv_x, conv_bc, norm_gain, w_out):
    R, K = tokens.shape
    N = w_xz.shape[2]
    HL = w_dt.shape[1]
    D = w_out.shape[1]
    bc = w_bc.shape[1]
    sw = bc // 2
    rows = R * n_head
    full = rows + HALO
    ny = n_head // 2
    kc, jc, pr = K // NK, D // NJ, N // 2 // NP
    V = pltpu.VMEM
    dma = pltpu.SemaphoreType.DMA
    vm = pl.BlockSpec(memory_space=pltpu.VMEM)
    anyspace = pl.BlockSpec(memory_space=pl.ANY)
    scratch = [
        V((NK, kc, 2, N), BF16), V((NJ, N, jc), BF16), V((K, bc), BF16), V((1, N), F32),
        V((rows, HL), F32), V((rows, HL), F32), V((rows, N), F32), V((full, K), BF16), V((full, 2 * kc), BF16),
        V((NK, rows, 2 * kc), BF16), V((rows, N), F32),
        V((256, 512), BF16), V((full, N), F32), V((full, bc), F32),
        V((rows, HL), F32), V((HL, rows), F32), V((HL, rows), F32),
        V((rows, N), BF16), V((rows, rows), F32),
        V((N, sw), F32), V((N, sw), BF16), V((NP, pr, sw), BF16), V((HL, 128), F32), V((HL, 128), F32),
        V((NP, pr, sw), BF16), V((NP, pr, sw), BF16), V((NP, pr, sw), BF16), V((N, sw), BF16),
        V((rows, N), F32), V((rows, N), BF16),
        V((ny, R, 128), F32), V((ny, R, 128), F32), V((ny, R, 128), F32), V((ny, R, 128), F32),
        V((ny, R, 128), F32),
        V((rows, jc), F32), V((NJ, ny, R, jc), BF16), V((NJ, ny, R, jc), BF16),
        V((NJ, ny, R, jc), BF16), V((NJ, ny, R, jc), BF16), V((NJ, ny, R, jc), F32),
        dma((NK,)), dma((NJ,)), dma, dma((n_head,)), dma, dma((NK,)), dma((NK,)),
        dma((ny, NK)), dma((ny, NK)), dma((ny, NK)), dma((ny, NK)),
        dma, dma, dma((NP,)), dma((NP,)), dma((NP,)), dma((NP,)), dma((NP,)), dma((NP,)),
        dma, dma, dma((ny,)), dma((ny,)), dma((NJ,)), dma((NJ,)), dma((NJ, ny)), dma((NJ, ny)),
    ]
    return pl.pallas_call(
        functools.partial(kernel, n_seq, n_head),
        out_shape=jax.ShapeDtypeStruct((R, D), BF16),
        in_specs=[vm, anyspace, anyspace, vm, vm, vm, vm, vm, vm, anyspace],
        out_specs=vm,
        scratch_shapes=scratch,
        compiler_params=pltpu.CompilerParams(
            collective_id=0, has_side_effects=True, vmem_limit_bytes=62 * 2**20),
    )(tokens, w_xz, w_bc, w_dt.T, dt_bias[None], a_log[None], conv_x, conv_bc, norm_gain, w_out)


def solution(mesh):
    in_specs = (
        P(("seq", "head"), None),
        P(None, None, "head"),
        P(),
        P(None, "head"),
        P("head"),
        P("head"),
        P(None, "head"),
        P(),
        P("head"),
        P("head", None),
    )
    out_specs = P(("seq", "head"), None)
    run = functools.partial(body, mesh.shape["seq"], mesh.shape["head"])
    return jax.shard_map(run, mesh=mesh, in_specs=in_specs, out_specs=out_specs, check_vma=False)
```
